32 devices in a mesh: leaf: 8 (over z, y), sub: 4 (over x, core).
Axes of the slice: x: 2, y: 2, z: 4, core: 2. Of those that a mesh axis runs over, the one named last changes fastest.
Arguments:
- signal: bfloat16 [32, 65536], P(None, ('leaf', 'sub')), may hold values from -6 to 6
- row_basis: bfloat16 [64, 65536], P(None, ('leaf', 'sub')), may hold values from -0.375 to 0.375
- transfer: bfloat16 [512, 9, 32, 128], P(('leaf', 'sub')), may hold values from -0.5 to 0.5
- column_basis: bfloat16 [64, 65536], P(None, ('leaf', 'sub')), may hold values from -0.75 to 0.75
- near_blocks: bfloat16 [768, 128, 256], P(('leaf', 'sub')), may hold values from -0.375 to 0.375
- near_list: int32 [768, 2], P(('leaf', 'sub')), may hold values from -1 to 31, as said below
Outputs:
- result: float32 [32, 65536], P(None, ('leaf', 'sub'))
The draws below stay inside these ranges and needn't reach their ends.
Inputs may be any that keep to these rules, and one draw needn't show every extreme that they name: `near_list`: on each device the live entries (column >= 0) fill a leading run of its 24 slots, 2 or more of them, and empty slots hold -1 in both places; a live entry has 0 <= column < 24 and column <= row <= column + 8. Devices 2m and 2m + 1 hold at most 24 live entries together, and some such pair holds 24.
All inputs are finite; a program needn't handle non-finite values.
Results may differ from the reference program's by a relative error of at most 0.0003.
Values may be sent and summed in bfloat16 or wider, within the bound.
A program may use at most 128 MiB of HBM per device.

```python
import jax
import jax.numpy as jnp
from jax import lax

BLOCK_RANK = 32
RHS = 16
LEAF = 128
BOX_DEV = 16
REACH = 4
CAP = 24
BUTTERFLY_DEPTH = 9
TOTAL_LEAF_BOXES = 512
NPTS = 65536
NEAR_SLOTS = 768
DEVICES = 32


def draw_near_list(key, part):
    pair_count = DEVICES // 2
    subkeys = jax.random.split(key, 6)
    heavy_count = jax.random.randint(subkeys[0], (pair_count,), CAP // 2, CAP - 1)
    full_pair = jax.random.randint(subkeys[1], (), 0, pair_count)
    heavy_count = jnp.where(jnp.arange(pair_count) == full_pair, CAP - 2, heavy_count)
    spare_room = CAP - heavy_count
    light_count = jax.random.randint(subkeys[2], (pair_count,), 2, spare_room + 1)
    heavy_first = jax.random.randint(subkeys[3], (pair_count,), 0, 2)
    first_count = jnp.where(heavy_first == 0, heavy_count, light_count)
    second_count = jnp.where(heavy_first == 0, light_count, heavy_count)
    counts = jnp.stack([first_count, second_count], axis=1).reshape(DEVICES)
    col_index = jax.random.randint(subkeys[4], (DEVICES, CAP), 0, BOX_DEV + 2 * REACH)
    offsets = jax.random.randint(subkeys[5], (DEVICES, CAP), 0, 2 * REACH + 1)
    slot_ids = jnp.arange(CAP)[None, :]
    col_index = jnp.where(slot_ids == 0, 0, col_index)
    offsets = jnp.where(slot_ids == 0, offsets % (2 * REACH), offsets)
    col_index = jnp.where(slot_ids == 1, BOX_DEV + 2 * REACH - 1, col_index)
    offsets = jnp.where(slot_ids == 1, 2 * REACH, offsets)
    row_index = col_index + offsets
    live_slot = slot_ids < counts[:, None]
    col_index = jnp.where(live_slot, col_index, -1)
    row_index = jnp.where(live_slot, row_index, -1)
    return jnp.stack([row_index, col_index], axis=-1).reshape(DEVICES * CAP, 2).astype(jnp.int32)


def shard_levels(own_key, extent, shards, smallest, high):
    def one(axis_at, parts):
        draws = jax.random.uniform(jax.random.fold_in(jax.random.fold_in(own_key, 6), axis_at), (parts,), jnp.float32, smallest / len(shards), high / len(shards))
        return jnp.repeat(jnp.exp(draws), extent[axis_at] // parts).reshape((-1,) + (1,) * (len(extent) - axis_at - 1))

    loudness = one(*shards[0])
    for cut in shards[1:]:
        loudness = loudness * one(*cut)
    return loudness


def gaussian(own_key, extent, deviation, reach, cuts=(), kind=jnp.bfloat16):
    level = shard_levels(own_key, extent, cuts, -0.22, 0.18) if cuts else 1.0
    drawn = jax.random.normal(own_key, extent, jnp.float32) * deviation * level
    return jnp.minimum(jnp.maximum(drawn, -reach), reach).astype(kind)


def setup_inputs(seed: int = 0) -> dict:
    streams_of = jax.random.split(jax.random.key(seed), 7)
    return {
        "signal": gaussian(streams_of[0], (2 * RHS, NPTS), 1.0, 6.0, ((1, 32),)),
        "row_basis": gaussian(streams_of[1], (2 * BLOCK_RANK, NPTS), (2 * LEAF) ** -0.5, 0.375, ((1, 32),)),
        "transfer": gaussian(streams_of[2], (TOTAL_LEAF_BOXES, BUTTERFLY_DEPTH, BLOCK_RANK, 4 * BLOCK_RANK), (4 * BLOCK_RANK) ** -0.5, 0.5, ((0, 32),)),
        "column_basis": gaussian(streams_of[3], (2 * BLOCK_RANK, NPTS), (2 * BLOCK_RANK) ** -0.5, 0.75, ((1, 32),)),
        "near_blocks": gaussian(streams_of[4], (NEAR_SLOTS, LEAF, 2 * LEAF), (2 * LEAF) ** -0.5, 0.375, ((0, 32),)),
        "near_list": draw_near_list(jax.random.fold_in(streams_of[6], 71), 0),
    }


highest = lax.Precision.HIGHEST


def project(signal, row_basis):
    rhs_count = signal.shape[0] // 2
    rank_width = row_basis.shape[0] // 2
    leaves = signal.shape[1] // LEAF
    samples = signal.astype(jnp.float32).reshape(2, rhs_count, leaves, LEAF)
    basis_rows = row_basis.astype(jnp.float32).reshape(2, rank_width, leaves, LEAF)
    products = jnp.einsum('xrlp,yqlp->xylrq', samples, basis_rows)
    real_part = products[0, 0] + products[1, 1]
    imag_part = products[1, 0] - products[0, 1]
    return jnp.transpose(jnp.concatenate([real_part, imag_part], axis=-1), (1, 0, 2))


def block_form(weights):
    matrices = weights.astype(jnp.float32)
    rank_width = matrices.shape[1]
    pieces = []
    for offspring in range(2):
        real_part = matrices[:, :, (2 * offspring) * rank_width:(2 * offspring + 1) * rank_width]
        imag_part = matrices[:, :, (2 * offspring + 1) * rank_width:(2 * offspring + 2) * rank_width]
        upper_rows = jnp.concatenate([real_part, -imag_part], axis=2)
        lower_rows = jnp.concatenate([imag_part, real_part], axis=2)
        pieces.append(jnp.concatenate([upper_rows, lower_rows], axis=1))
    return jnp.concatenate(pieces, axis=1)


def apply_level(paired, weights):
    return jnp.einsum('rsm,smn->rsn', paired, block_form(weights), precision=highest)


def pair_local(coeffs, height):
    rhs_count, slot_count, doubled = coeffs.shape
    half_span = 2 ** (height - 1)
    grouped = coeffs.reshape(rhs_count, slot_count // (2 * half_span), 2, half_span, doubled)
    joined = jnp.concatenate([grouped[:, :, 0], grouped[:, :, 1]], axis=-1)
    twice = jnp.stack([joined, joined], axis=2)
    return twice.reshape(rhs_count, slot_count, 2 * doubled)


def evaluate(coeffs, column_basis):
    rhs_count, leaves, doubled = coeffs.shape
    rank_width = doubled // 2
    basis_rows = column_basis.astype(jnp.float32).reshape(2, rank_width, leaves, LEAF)
    real_coefficient = coeffs[:, :, :rank_width]
    imag_coef = coeffs[:, :, rank_width:]
    real_out = (jnp.einsum('rlq,qlp->rlp', real_coefficient, basis_rows[0], precision=highest)
                - jnp.einsum('rlq,qlp->rlp', imag_coef, basis_rows[1], precision=highest))
    imag_out = (jnp.einsum('rlq,qlp->rlp', imag_coef, basis_rows[0], precision=highest)
                + jnp.einsum('rlq,qlp->rlp', real_coefficient, basis_rows[1], precision=highest))
    return jnp.concatenate([real_out, imag_out], axis=0).reshape(2 * rhs_count, leaves * LEAF)


def pick_rows(window, row_index):
    channels = window.shape[0]
    leaf_tiles = window.reshape(channels, -1, LEAF)
    picked = jnp.take(leaf_tiles, jnp.maximum(row_index, 0), axis=1)
    return jnp.transpose(picked, (1, 0, 2))


def near_products(picked, blocks):
    products = jnp.einsum('scp,spj->scj', picked.astype(jnp.float32), blocks.astype(jnp.float32))
    rhs_count = picked.shape[1] // 2
    real_part = products[:, :rhs_count, :LEAF] + products[:, rhs_count:, LEAF:]
    imag_part = products[:, rhs_count:, :LEAF] - products[:, :rhs_count, LEAF:]
    return jnp.concatenate([real_part, imag_part], axis=1)


def accumulate(output_values, col_index, box_count):
    selector = (col_index[:, None] == jnp.arange(box_count, dtype=jnp.int32)[None, :]).astype(jnp.float32)
    return jnp.einsum('sw,scj->cwj', selector, output_values, precision=highest)


def near_field(signal, near_blocks, near_list):
    channels = signal.shape[0]
    window_width = (BOX_DEV + 4 * REACH) * LEAF
    edge_width = 2 * REACH * LEAF
    extended = jnp.concatenate([signal[:, -edge_width:], signal, signal[:, :edge_width]], axis=1)
    blocks = near_blocks.reshape(DEVICES, CAP, LEAF, 2 * LEAF)
    entries = near_list.reshape(DEVICES, CAP, 2)

    def one_device(item_data):
        device, dev_blocks, dev_entries = item_data
        window = lax.dynamic_slice_in_dim(extended, device * (BOX_DEV * LEAF), window_width, 1)
        picked = pick_rows(window, dev_entries[:, 0])
        return accumulate(near_products(picked, dev_blocks), dev_entries[:, 1], BOX_DEV + 2 * REACH)

    windows = lax.map(one_device, (jnp.arange(DEVICES, dtype=jnp.int32), blocks, entries))
    center = windows[:, :, REACH:REACH + BOX_DEV]
    left_rim = windows[:, :, :REACH]
    right_rim = windows[:, :, BOX_DEV + REACH:]
    center = center.at[:, :, BOX_DEV - REACH:].add(jnp.roll(left_rim, -1, axis=0))
    center = center.at[:, :, :REACH].add(jnp.roll(right_rim, 1, axis=0))
    return jnp.transpose(center, (1, 0, 2, 3)).reshape(channels, DEVICES * BOX_DEV * LEAF)


def reference(signal, row_basis, transfer, column_basis, near_blocks, near_list):
    coeffs = project(signal, row_basis)
    for height in range(1, BUTTERFLY_DEPTH + 1):
        coeffs = apply_level(pair_local(coeffs, height), transfer[:, height - 1])
    far_field = evaluate(coeffs, column_basis)
    return far_field + near_field(signal, near_blocks, near_list)
```

```python
import functools

import jax
import jax.numpy as jnp
from jax import lax
from jax.experimental import pallas as pl
from jax.experimental.pallas import tpu as pltpu
from jax.sharding import PartitionSpec as P

LEAF = 128
MESH = pl.DeviceIdType.MESH
F32 = jnp.float32
BF16 = jnp.bfloat16
CHUNKS = 2


def dot(a, b):
    return lax.dot_general(a, b, (((1,), (0,)), ((), ())), preferred_element_type=F32)


def dot_t(a, b):
    return lax.dot_general(a, b, (((1,), (1,)), ((), ())), preferred_element_type=F32)


def halves(value):
    high = value.astype(BF16)
    low = (value - high.astype(F32)).astype(BF16)
    return high, low


def product(value, matrix):
    rows = value.shape[0]
    both = dot(jnp.concatenate(halves(value), axis=0), matrix)
    return both[:rows] + both[rows:]


def kernel(
    leaf_count, sub_count,
    list_ref, signal_hbm, row_hbm, transfer_hbm, column_hbm, block_hbm, out_ref,
    win, row_basis, transfer, column_basis, blocks, spread, evals, sent, got, own, vals, near, edges,
    in_sems, send_sems, recv_sems, halo_send, halo_recv,
):
    boxes = signal_hbm.shape[1] // LEAF
    channels = signal_hbm.shape[0]
    rhs = channels // 2
    rank = row_hbm.shape[0] // 2
    wide = 2 * rank
    reach = boxes // 4
    pairs = boxes // 2
    local_levels = boxes.bit_length() - 1
    slots = block_hbm.shape[0]
    levels = transfer_hbm.shape[1]
    leaf = lax.axis_index("leaf")
    sub = lax.axis_index("sub")
    count = leaf_count * sub_count
    me = leaf * sub_count + sub
    after = lax.rem(me + 1, count)
    before = lax.rem(me + count - 1, count)
    next_id = (lax.div(after, sub_count), lax.rem(after, sub_count))
    prev_id = (lax.div(before, sub_count), lax.rem(before, sub_count))

    crossing = []
    for place in range(sub_count.bit_length() - 1):
        bit = lax.rem(lax.div(sub, 1 << place), 2)
        crossing.append((bit, (leaf, sub + (1 - 2 * bit) * (1 << place))))
    for place in range(leaf_count.bit_length() - 1):
        bit = lax.rem(lax.div(leaf, 1 << place), 2)
        crossing.append((bit, (leaf + (1 - 2 * bit) * (1 << place), sub)))
    partners = [partner for _, partner in crossing] + [next_id, prev_id]

    signal_copies = [
        pltpu.make_async_copy(
            signal_hbm.at[:, pl.ds(b * LEAF, LEAF)], win.at[2 * reach + b], in_sems.at[b]
        )
        for b in range(boxes)
    ]
    row_copy = pltpu.make_async_copy(row_hbm, row_basis, in_sems.at[boxes])
    column_copy = pltpu.make_async_copy(column_hbm, column_basis, in_sems.at[boxes + 1])
    block_copy = pltpu.make_async_copy(block_hbm, blocks, in_sems.at[boxes + 2])
    transfer_copies = [
        pltpu.make_async_copy(transfer_hbm.at[:, l], transfer.at[l], in_sems.at[boxes + 3 + l])
        for l in range(levels)
    ]
    for copy in signal_copies:
        copy.start()
    row_copy.start()
    for l in range(local_levels):
        transfer_copies[l].start()

    barrier = pltpu.get_barrier_semaphore()
    for partner in partners:
        pl.semaphore_signal(barrier, inc=1, device_id=partner, device_id_type=MESH)
    for l in range(local_levels, levels):
        transfer_copies[l].start()
    block_copy.start()
    column_copy.start()

    source = lax.broadcasted_iota(jnp.int32, (LEAF, 4 * LEAF), 0)
    target = lax.broadcasted_iota(jnp.int32, (LEAF, 4 * LEAF), 1)
    group = target // LEAF
    child = group // 2
    lower = group % 2
    lane = target % LEAF
    inner = lane % wide
    imag = inner // rank
    moved = inner + lower * (rank - 2 * rank * imag)
    sign = (1 - 2 * imag * (1 - lower)).astype(F32)
    hit = source == child * wide + moved
    moves = [
        jnp.where(hit & (lane // wide == half), sign, 0.0).astype(BF16) for half in range(2)
    ]

    def build(l):
        transfer_copies[l].wait()
        forms = []
        for half in range(2):
            weights = transfer[l, half * pairs : (half + 1) * pairs].reshape(pairs * rank, LEAF)
            forms.append(dot(weights, moves[half]))
        if l == local_levels - 1:
            full = (forms[0] + forms[1]).astype(BF16).reshape(pairs, rank, 4 * LEAF)
            for g in range(4):
                spread[l, 0, :, g * rank : (g + 1) * rank, :] = full[
                    :, :, g * LEAF : (g + 1) * LEAF
                ]
            return
        for half in range(2):
            form = forms[half].astype(BF16).reshape(pairs, rank, 4 * LEAF)
            for c in range(2):
                for part in range(2):
                    top = half * wide + part * rank
                    g = 2 * c + part
                    spread[l, c, :, top : top + rank, :] = form[:, :, g * LEAF : (g + 1) * LEAF]

    left = lax.broadcasted_iota(jnp.int32, (rhs, LEAF), 1) < wide

    for copy in signal_copies:
        copy.wait()
    pl.semaphore_wait(barrier, len(partners))
    halo = [
        pltpu.make_async_remote_copy(
            src_ref=win.at[pl.ds(boxes, 2 * reach)], dst_ref=win.at[pl.ds(0, 2 * reach)],
            send_sem=halo_send.at[0], recv_sem=halo_recv.at[0],
            device_id=next_id, device_id_type=MESH,
        ),
        pltpu.make_async_remote_copy(
            src_ref=win.at[pl.ds(2 * reach, 2 * reach)],
            dst_ref=win.at[pl.ds(2 * reach + boxes, 2 * reach)],
            send_sem=halo_send.at[1], recv_sem=halo_recv.at[1],
            device_id=prev_id, device_id_type=MESH,
        ),
    ]
    for copy in halo:
        copy.start()

    row_copy.wait()
    coeffs = []
    for k in range(pairs):
        real_side, imag_side = [], []
        for b in (k, k + pairs):
            basis = row_basis[:, b * LEAF : (b + 1) * LEAF]
            real_side += [basis[:rank], -basis[rank:]]
            imag_side += [basis[rank:], basis[:rank]]
        points = [win[2 * reach + b] for b in (k, k + pairs)]
        both = dot_t(
            jnp.concatenate([points[0][:rhs], points[1][:rhs]], axis=0),
            jnp.concatenate(real_side, axis=0),
        ) + dot_t(
            jnp.concatenate([points[0][rhs:], points[1][rhs:]], axis=0),
            jnp.concatenate(imag_side, axis=0),
        )
        coeffs.append(jnp.where(left, both[:rhs], both[rhs:]))

    for l in range(local_levels):
        build(l)
    for l in range(local_levels - 1):
        bit = 1 << l
        coeffs = [
            product(coeffs[k & ~bit], spread[l, 0, k]) + product(coeffs[k | bit], spread[l, 1, k])
            for k in range(pairs)
        ]
    last = local_levels - 1
    coeffs = [product(coeffs[k], spread[last, 0, k]) for k in range(pairs)]

    chunk = pairs // CHUNKS

    def exchange(i, part):
        span = pl.ds(part * chunk, chunk)
        return pltpu.make_async_remote_copy(
            src_ref=sent.at[i, span], dst_ref=got.at[i, span],
            send_sem=send_sems.at[i, part], recv_sem=recv_sems.at[i, part],
            device_id=crossing[i][1], device_id_type=MESH,
        )

    def near_products():
        for copy in halo:
            copy.wait_recv()
        block_copy.wait()
        for s in range(slots):
            picked = win[jnp.maximum(list_ref[s, 0], 0)]
            both = dot(picked, blocks[s])
            vals[s, :rhs] = both[:rhs, :LEAF] + both[rhs:, LEAF:]
            vals[s, rhs:] = both[rhs:, :LEAF] - both[:rhs, LEAF:]

    def near_sum(j):
        total = jnp.zeros((channels, LEAF), F32)
        for s in range(slots):
            total = total + jnp.where(list_ref[s, 1] == j, vals[s], 0.0)
        near[j] = total

    def near_sums(first, stop):
        def body(j, carry):
            near_sum(j)
            return carry

        lax.fori_loop(first, stop, body, 0)

    rim = [
        pltpu.make_async_remote_copy(
            src_ref=near.at[pl.ds(0, reach)], dst_ref=edges.at[1],
            send_sem=halo_send.at[2], recv_sem=halo_recv.at[2],
            device_id=prev_id, device_id_type=MESH,
        ),
        pltpu.make_async_remote_copy(
            src_ref=near.at[pl.ds(boxes + reach, reach)], dst_ref=edges.at[0],
            send_sem=halo_send.at[3], recv_sem=halo_recv.at[3],
            device_id=next_id, device_id_type=MESH,
        ),
    ]

    def near_edges():
        near_products()
        near_sums(0, reach)
        rim[0].start()
        near_sums(boxes + reach, boxes + 2 * reach)
        rim[1].start()

    def near_middle():
        near_sums(reach, boxes + reach)

    def build_evals():
        column_copy.wait()
        for k in range(pairs):
            for half in range(2):
                b = k + half * pairs
                basis = column_basis[:, b * LEAF : (b + 1) * LEAF]
                top = half * wide
                evals[k, top : top + rank, :LEAF] = basis[:rank]
                evals[k, top : top + rank, LEAF:] = basis[rank:]
                evals[k, top + rank : top + wide, :LEAF] = -basis[rank:]
                evals[k, top + rank : top + wide, LEAF:] = basis[:rank]

    steps = len(crossing)
    extra = [[] for _ in range(steps)]
    extra[min(1, steps - 1)].append(near_edges)
    extra[min(2, steps - 1)].append(near_middle)
    extra[min(3, steps - 1)].append(build_evals)

    for part in range(CHUNKS):
        for k in range(part * chunk, (part + 1) * chunk):
            sent[0, k] = coeffs[k]
        exchange(0, part).start()
    for i in range(steps):
        l = local_levels + i
        bit = crossing[i][0]
        build(l)
        for k in range(pairs):
            own[k] = product(sent[i, k], spread[l, bit, k])
        for work in extra[i]:
            work()
        if i == steps - 1:
            for copy in rim:
                copy.wait_recv()
        for part in range(CHUNKS):
            exchange(i, part).wait_recv()
            for k in range(part * chunk, (part + 1) * chunk):
                value = own[k] + product(got[i, k], spread[l, 1 - bit, k])
                if i < steps - 1:
                    sent[i + 1, k] = value
                    continue
                high, low = halves(value)
                zero = jnp.zeros_like(high)
                far = dot(
                    jnp.concatenate(
                        [
                            jnp.where(left, high, zero), jnp.where(left, low, zero),
                            jnp.where(left, zero, high), jnp.where(left, zero, low),
                        ],
                        axis=0,
                    ),
                    evals[k],
                )
                for half in range(2):
                    b = k + half * pairs
                    both = far[2 * half * rhs : (2 * half + 1) * rhs] + far[
                        (2 * half + 1) * rhs : (2 * half + 2) * rhs
                    ]
                    result = near[reach + b]
                    if b < reach:
                        result = result + edges[0, b]
                    if b >= boxes - reach:
                        result = result + edges[1, b - boxes + reach]
                    here = slice(b * LEAF, (b + 1) * LEAF)
                    out_ref[:rhs, here] = both[:, :LEAF] + result[:rhs]
                    out_ref[rhs:, here] = both[:, LEAF:] + result[rhs:]
            if i < steps - 1:
                exchange(i + 1, part).start()
    for i in range(steps):
        for part in range(CHUNKS):
            exchange(i, part).wait_send()
    for copy in halo + rim:
        copy.wait_send()


def solution(mesh):
    leaf_count, sub_count = mesh.shape["leaf"], mesh.shape["sub"]
    steps = leaf_count.bit_length() + sub_count.bit_length() - 2

    def shards(signal, row_basis, transfer, column_basis, near_blocks, near_list):
        channels, points = signal.shape
        boxes = points // LEAF
        reach, pairs = boxes // 4, boxes // 2
        rhs = channels // 2
        levels, rank = transfer.shape[1], transfer.shape[2]
        slots = near_blocks.shape[0]
        anywhere = pl.BlockSpec(memory_space=pl.ANY)
        return pl.pallas_call(
            functools.partial(kernel, leaf_count, sub_count),
            out_shape=jax.ShapeDtypeStruct((channels, points), F32),
            in_specs=[pl.BlockSpec(memory_space=pltpu.SMEM)] + [anywhere] * 5,
            out_specs=pl.BlockSpec(memory_space=pltpu.VMEM),
            scratch_shapes=[
                pltpu.VMEM((boxes + 4 * reach, channels, LEAF), BF16),
                pltpu.VMEM(row_basis.shape, BF16),
                pltpu.VMEM((levels, boxes, rank, LEAF), BF16),
                pltpu.VMEM(column_basis.shape, BF16),
                pltpu.VMEM(near_blocks.shape, BF16),
                pltpu.VMEM((levels, 2, pairs, LEAF, LEAF), BF16),
                pltpu.VMEM((pairs, LEAF, 2 * LEAF), BF16),
                pltpu.VMEM((steps, pairs, rhs, LEAF), F32),
                pltpu.VMEM((steps, pairs, rhs, LEAF), F32),
                pltpu.VMEM((pairs, rhs, LEAF), F32),
                pltpu.VMEM((slots, channels, LEAF), F32),
                pltpu.VMEM((boxes + 2 * reach, channels, LEAF), F32),
                pltpu.VMEM((2, reach, channels, LEAF), F32),
                pltpu.SemaphoreType.DMA((boxes + 3 + levels,)),
                pltpu.SemaphoreType.DMA((steps, CHUNKS)),
                pltpu.SemaphoreType.DMA((steps, CHUNKS)),
                pltpu.SemaphoreType.DMA((4,)),
                pltpu.SemaphoreType.DMA((4,)),
            ],
            compiler_params=pltpu.CompilerParams(
                collective_id=0, has_side_effects=True, vmem_limit_bytes=40 * 1024 * 1024
            ),
        )(near_list, signal, row_basis, transfer, column_basis, near_blocks)

    return jax.shard_map(
        shards,
        mesh=mesh,
        in_specs=(
            P(None, ("leaf", "sub")),
            P(None, ("leaf", "sub")),
            P(("leaf", "sub"), None, None, None),
            P(None, ("leaf", "sub")),
            P(("leaf", "sub"), None, None),
            P(("leaf", "sub"), None),
        ),
        out_specs=P(None, ("leaf", "sub")),
        check_vma=False,
    )
```

```python
import functools

import jax
import jax.numpy as jnp
from jax import lax
from jax.experimental import pallas as pl
from jax.experimental.pallas import tpu as pltpu
from jax.sharding import PartitionSpec as P

LEAF = 128
MESH = pl.DeviceIdType.MESH
F32 = jnp.float32
BF16 = jnp.bfloat16
CHUNKS = 2


def dot(a, b):
    return lax.dot_general(a, b, (((1,), (0,)), ((), ())), preferred_element_type=F32)


def dot_t(a, b):
    return lax.dot_general(a, b, (((1,), (1,)), ((), ())), preferred_element_type=F32)


def halves(value):
    high = value.astype(BF16)
    low = (value - high.astype(F32)).astype(BF16)
    return high, low


def product(value, matrix):
    rows = value.shape[0]
    both = dot(jnp.concatenate(halves(value), axis=0), matrix)
    return both[:rows] + both[rows:]


def kernel(
    leaf_count, sub_count,
    list_ref, signal_hbm, row_hbm, transfer_hbm, column_hbm, block_hbm, out_ref,
    win, row_basis, transfer, column_basis, blocks, spread, evals, sent, got, own, vals, near, edges,
    in_sems, send_sems, recv_sems, halo_send, halo_recv,
):
    boxes = signal_hbm.shape[1] // LEAF
    channels = signal_hbm.shape[0]
    rhs = channels // 2
    rank = row_hbm.shape[0] // 2
    wide = 2 * rank
    reach = boxes // 4
    pairs = boxes // 2
    local_levels = boxes.bit_length() - 1
    slots = block_hbm.shape[0]
    levels = transfer_hbm.shape[1]
    leaf = lax.axis_index("leaf")
    sub = lax.axis_index("sub")
    count = leaf_count * sub_count
    me = leaf * sub_count + sub
    after = lax.rem(me + 1, count)
    before = lax.rem(me + count - 1, count)
    next_id = (lax.div(after, sub_count), lax.rem(after, sub_count))
    prev_id = (lax.div(before, sub_count), lax.rem(before, sub_count))

    crossing = []
    for place in range(sub_count.bit_length() - 1):
        bit = lax.rem(lax.div(sub, 1 << place), 2)
        crossing.append((bit, (leaf, sub + (1 - 2 * bit) * (1 << place))))
    for place in range(leaf_count.bit_length() - 1):
        bit = lax.rem(lax.div(leaf, 1 << place), 2)
        crossing.append((bit, (leaf + (1 - 2 * bit) * (1 << place), sub)))
    partners = [partner for _, partner in crossing] + [next_id, prev_id]

    signal_copies = [
        pltpu.make_async_copy(
            signal_hbm.at[:, pl.ds(b * LEAF, LEAF)], win.at[2 * reach + b], in_sems.at[b]
        )
        for b in range(boxes)
    ]
    row_copy = pltpu.make_async_copy(row_hbm, row_basis, in_sems.at[boxes])
    column_copy = pltpu.make_async_copy(column_hbm, column_basis, in_sems.at[boxes + 1])
    block_copy = pltpu.make_async_copy(block_hbm, blocks, in_sems.at[boxes + 2])
    transfer_copies = [
        pltpu.make_async_copy(transfer_hbm.at[:, l], transfer.at[l], in_sems.at[boxes + 3 + l])
        for l in range(levels)
    ]
    for copy in signal_copies:
        copy.start()
    row_copy.start()
    for l in range(local_levels):
        transfer_copies[l].start()

    barrier = pltpu.get_barrier_semaphore()
    for partner in partners:
        pl.semaphore_signal(barrier, inc=1, device_id=partner, device_id_type=MESH)
    for l in range(local_levels, levels):
        transfer_copies[l].start()
    block_copy.start()
    column_copy.start()

    source = lax.broadcasted_iota(jnp.int32, (LEAF, 4 * LEAF), 0)
    target = lax.broadcasted_iota(jnp.int32, (LEAF, 4 * LEAF), 1)
    group = target // LEAF
    child = group // 2
    lower = group % 2
    lane = target % LEAF
    inner = lane % wide
    imag = inner // rank
    moved = inner + lower * (rank - 2 * rank * imag)
    sign = (1 - 2 * imag * (1 - lower)).astype(F32)
    hit = source == child * wide + moved
    moves = [
        jnp.where(hit & (lane // wide == half), sign, 0.0).astype(BF16) for half in range(2)
    ]

    def build(l):
        transfer_copies[l].wait()
        forms = []
        for half in range(2):
            weights = transfer[l, half * pairs : (half + 1) * pairs].reshape(pairs * rank, LEAF)
            forms.append(dot(weights, moves[half]))
        if l == local_levels - 1:
            full = (forms[0] + forms[1]).astype(BF16).reshape(pairs, rank, 4 * LEAF)
            for g in range(4):
                spread[l, 0, :, g * rank : (g + 1) * rank, :] = full[
                    :, :, g * LEAF : (g + 1) * LEAF
                ]
            return
        for half in range(2):
            form = forms[half].astype(BF16).reshape(pairs, rank, 4 * LEAF)
            for c in range(2):
                for part in range(2):
                    top = half * wide + part * rank
                    g = 2 * c + part
                    spread[l, c, :, top : top + rank, :] = form[:, :, g * LEAF : (g + 1) * LEAF]

    left = lax.broadcasted_iota(jnp.int32, (rhs, LEAF), 1) < wide

    for copy in signal_copies:
        copy.wait()
    pl.semaphore_wait(barrier, len(partners))
    halo = [
        pltpu.make_async_remote_copy(
            src_ref=win.at[pl.ds(boxes, 2 * reach)], dst_ref=win.at[pl.ds(0, 2 * reach)],
            send_sem=halo_send.at[0], recv_sem=halo_recv.at[0],
            device_id=next_id, device_id_type=MESH,
        ),
        pltpu.make_async_remote_copy(
            src_ref=win.at[pl.ds(2 * reach, 2 * reach)],
            dst_ref=win.at[pl.ds(2 * reach + boxes, 2 * reach)],
            send_sem=halo_send.at[1], recv_sem=halo_recv.at[1],
            device_id=prev_id, device_id_type=MESH,
        ),
    ]
    for copy in halo:
        copy.start()

    row_copy.wait()
    coeffs = []
    for k in range(pairs):
        real_side, imag_side = [], []
        for b in (k, k + pairs):
            basis = row_basis[:, b * LEAF : (b + 1) * LEAF]
            real_side += [basis[:rank], -basis[rank:]]
            imag_side += [basis[rank:], basis[:rank]]
        points = [win[2 * reach + b] for b in (k, k + pairs)]
        both = dot_t(
            jnp.concatenate([points[0][:rhs], points[1][:rhs]], axis=0),
            jnp.concatenate(real_side, axis=0),
        ) + dot_t(
            jnp.concatenate([points[0][rhs:], points[1][rhs:]], axis=0),
            jnp.concatenate(imag_side, axis=0),
        )
        coeffs.append(jnp.where(left, both[:rhs], both[rhs:]))

    for l in range(local_levels):
        build(l)
    for l in range(local_levels - 1):
        bit = 1 << l
        coeffs = [
            product(coeffs[k & ~bit], spread[l, 0, k]) + product(coeffs[k | bit], spread[l, 1, k])
            for k in range(pairs)
        ]
    last = local_levels - 1
    coeffs = [product(coeffs[k], spread[last, 0, k]) for k in range(pairs)]

    chunk = pairs // CHUNKS

    def exchange(i, part):
        span = pl.ds(part * chunk, chunk)
        return pltpu.make_async_remote_copy(
            src_ref=sent.at[i, span], dst_ref=got.at[i, span],
            send_sem=send_sems.at[i, part], recv_sem=recv_sems.at[i, part],
            device_id=crossing[i][1], device_id_type=MESH,
        )

    def near_products():
        for copy in halo:
            copy.wait_recv()
        block_copy.wait()
        for s in range(slots):
            picked = win[jnp.maximum(list_ref[0, s], 0)]
            both = dot(picked, blocks[s])
            vals[s, :rhs] = both[:rhs, :LEAF] + both[rhs:, LEAF:]
            vals[s, rhs:] = both[rhs:, :LEAF] - both[:rhs, LEAF:]

    def near_sum(j):
        total = jnp.zeros((channels, LEAF), F32)
        for s in range(slots):
            total = total + jnp.where(list_ref[1, s] == j, vals[s], 0.0)
        near[j] = total

    def near_sums(first, stop):
        def body(j, carry):
            near_sum(j)
            return carry

        lax.fori_loop(first, stop, body, 0)

    rim = [
        pltpu.make_async_remote_copy(
            src_ref=near.at[pl.ds(0, reach)], dst_ref=edges.at[1],
            send_sem=halo_send.at[2], recv_sem=halo_recv.at[2],
            device_id=prev_id, device_id_type=MESH,
        ),
        pltpu.make_async_remote_copy(
            src_ref=near.at[pl.ds(boxes + reach, reach)], dst_ref=edges.at[0],
            send_sem=halo_send.at[3], recv_sem=halo_recv.at[3],
            device_id=next_id, device_id_type=MESH,
        ),
    ]

    def near_edges():
        near_products()
        near_sums(0, reach)
        rim[0].start()
        near_sums(boxes + reach, boxes + 2 * reach)
        rim[1].start()

    def near_middle():
        near_sums(reach, boxes + reach)

    def build_evals():
        column_copy.wait()
        for k in range(pairs):
            for half in range(2):
                b = k + half * pairs
                basis = column_basis[:, b * LEAF : (b + 1) * LEAF]
                top = half * wide
                evals[k, top : top + rank, :LEAF] = basis[:rank]
                evals[k, top : top + rank, LEAF:] = basis[rank:]
                evals[k, top + rank : top + wide, :LEAF] = -basis[rank:]
                evals[k, top + rank : top + wide, LEAF:] = basis[:rank]

    steps = len(crossing)
    extra = [[] for _ in range(steps)]
    extra[min(1, steps - 1)].append(near_edges)
    extra[min(2, steps - 1)].append(near_middle)
    extra[min(3, steps - 1)].append(build_evals)

    for part in range(CHUNKS):
        for k in range(part * chunk, (part + 1) * chunk):
            sent[0, k] = coeffs[k]
        exchange(0, part).start()
    for i in range(steps):
        l = local_levels + i
        bit = crossing[i][0]
        build(l)
        for k in range(pairs):
            own[k] = product(sent[i, k], spread[l, bit, k])
        for work in extra[i]:
            work()
        if i == steps - 1:
            for copy in rim:
                copy.wait_recv()
        for part in range(CHUNKS):
            exchange(i, part).wait_recv()
            for k in range(part * chunk, (part + 1) * chunk):
                value = own[k] + product(got[i, k], spread[l, 1 - bit, k])
                if i < steps - 1:
                    sent[i + 1, k] = value
                    continue
                high, low = halves(value)
                zero = jnp.zeros_like(high)
                far = dot(
                    jnp.concatenate(
                        [
                            jnp.where(left, high, zero), jnp.where(left, low, zero),
                            jnp.where(left, zero, high), jnp.where(left, zero, low),
                        ],
                        axis=0,
                    ),
                    evals[k],
                )
                for half in range(2):
                    b = k + half * pairs
                    both = far[2 * half * rhs : (2 * half + 1) * rhs] + far[
                        (2 * half + 1) * rhs : (2 * half + 2) * rhs
                    ]
                    result = near[reach + b]
                    if b < reach:
                        result = result + edges[0, b]
                    if b >= boxes - reach:
                        result = result + edges[1, b - boxes + reach]
                    here = slice(b * LEAF, (b + 1) * LEAF)
                    out_ref[:rhs, here] = both[:, :LEAF] + result[:rhs]
                    out_ref[rhs:, here] = both[:, LEAF:] + result[rhs:]
            if i < steps - 1:
                exchange(i + 1, part).start()
    for i in range(steps):
        for part in range(CHUNKS):
            exchange(i, part).wait_send()
    for copy in halo + rim:
        copy.wait_send()


def solution(mesh):
    leaf_count, sub_count = mesh.shape["leaf"], mesh.shape["sub"]
    steps = leaf_count.bit_length() + sub_count.bit_length() - 2

    def shards(signal, row_basis, transfer, column_basis, near_blocks, near_list):
        channels, points = signal.shape
        boxes = points // LEAF
        reach, pairs = boxes // 4, boxes // 2
        rhs = channels // 2
        levels, rank = transfer.shape[1], transfer.shape[2]
        slots = near_blocks.shape[0]
        anywhere = pl.BlockSpec(memory_space=pltpu.HBM)
        return pl.pallas_call(
            functools.partial(kernel, leaf_count, sub_count),
            out_shape=jax.ShapeDtypeStruct((channels, points), F32),
            in_specs=[pl.BlockSpec(memory_space=pltpu.SMEM)] + [anywhere] * 5,
            out_specs=pl.BlockSpec(memory_space=pltpu.VMEM),
            scratch_shapes=[
                pltpu.VMEM((boxes + 4 * reach, channels, LEAF), BF16),
                pltpu.VMEM(row_basis.shape, BF16),
                pltpu.VMEM((levels, boxes, rank, LEAF), BF16),
                pltpu.VMEM(column_basis.shape, BF16),
                pltpu.VMEM(near_blocks.shape, BF16),
                pltpu.VMEM((levels, 2, pairs, LEAF, LEAF), BF16),
                pltpu.VMEM((pairs, LEAF, 2 * LEAF), BF16),
                pltpu.VMEM((steps, pairs, rhs, LEAF), F32),
                pltpu.VMEM((steps, pairs, rhs, LEAF), F32),
                pltpu.VMEM((pairs, rhs, LEAF), F32),
                pltpu.VMEM((slots, channels, LEAF), F32),
                pltpu.VMEM((boxes + 2 * reach, channels, LEAF), F32),
                pltpu.VMEM((2, reach, channels, LEAF), F32),
                pltpu.SemaphoreType.DMA((boxes + 3 + levels,)),
                pltpu.SemaphoreType.DMA((steps, CHUNKS)),
                pltpu.SemaphoreType.DMA((steps, CHUNKS)),
                pltpu.SemaphoreType.DMA((4,)),
                pltpu.SemaphoreType.DMA((4,)),
            ],
            compiler_params=pltpu.CompilerParams(
                collective_id=0, has_side_effects=True, vmem_limit_bytes=63000000
            ),
        )(near_list.T, signal, row_basis, transfer, column_basis, near_blocks)

    return jax.shard_map(
        shards,
        mesh=mesh,
        in_specs=(
            P(None, ("leaf", "sub")),
            P(None, ("leaf", "sub")),
            P(("leaf", "sub"), None, None, None),
            P(None, ("leaf", "sub")),
            P(("leaf", "sub"), None, None),
            P(("leaf", "sub"), None),
        ),
        out_specs=P(None, ("leaf", "sub")),
        check_vma=False,
    )
```

```python
import functools

import jax
import jax.numpy as jnp
from jax import lax
from jax.experimental import pallas as pl
from jax.experimental.pallas import tpu as pltpu
from jax.sharding import PartitionSpec as P

LEAF = 128
MESH = pl.DeviceIdType.MESH
F32 = jnp.float32
BF16 = jnp.bfloat16
CHUNKS = 2


def dot(a, b):
    return lax.dot_general(a, b, (((1,), (0,)), ((), ())), preferred_element_type=F32)


def dot_t(a, b):
    return lax.dot_general(a, b, (((1,), (1,)), ((), ())), preferred_element_type=F32)


def halves(value):
    high = value.astype(BF16)
    low = (value - high.astype(F32)).astype(BF16)
    return high, low


def product(value, matrix):
    rows = value.shape[0]
    both = dot(jnp.concatenate(halves(value), axis=0), matrix)
    return both[:rows] + both[rows:]


def kernel(
    leaf_count, sub_count,
    list_ref, signal_hbm, row_hbm, transfer_hbm, column_hbm, block_hbm, out_ref,
    win, row_basis, transfer, column_basis, blocks, spread, evals, sent, got, own, vals, near, edges,
    in_sems, send_sems, recv_sems, halo_send, halo_recv,
):
    boxes = signal_hbm.shape[1] // LEAF
    channels = signal_hbm.shape[0]
    rhs = channels // 2
    rank = row_hbm.shape[0] // 2
    wide = 2 * rank
    reach = boxes // 4
    pairs = boxes // 2
    local_levels = boxes.bit_length() - 1
    slots = block_hbm.shape[0]
    levels = transfer_hbm.shape[1]
    leaf = lax.axis_index("leaf")
    sub = lax.axis_index("sub")
    count = leaf_count * sub_count
    me = leaf * sub_count + sub
    after = lax.rem(me + 1, count)
    before = lax.rem(me + count - 1, count)
    next_id = (lax.div(after, sub_count), lax.rem(after, sub_count))
    prev_id = (lax.div(before, sub_count), lax.rem(before, sub_count))

    crossing = []
    for place in range(sub_count.bit_length() - 1):
        bit = lax.rem(lax.div(sub, 1 << place), 2)
        crossing.append((bit, (leaf, sub + (1 - 2 * bit) * (1 << place))))
    for place in range(leaf_count.bit_length() - 1):
        bit = lax.rem(lax.div(leaf, 1 << place), 2)
        crossing.append((bit, (leaf + (1 - 2 * bit) * (1 << place), sub)))
    partners = [partner for _, partner in crossing] + [next_id, prev_id]

    signal_copies = [
        pltpu.make_async_copy(
            signal_hbm.at[:, pl.ds(b * LEAF, LEAF)], win.at[2 * reach + b], in_sems.at[b]
        )
        for b in range(boxes)
    ]
    row_copy = pltpu.make_async_copy(row_hbm, row_basis, in_sems.at[boxes])
    column_copy = pltpu.make_async_copy(column_hbm, column_basis, in_sems.at[boxes + 1])
    block_copy = pltpu.make_async_copy(block_hbm, blocks, in_sems.at[boxes + 2])
    transfer_copies = [
        pltpu.make_async_copy(transfer_hbm.at[:, l], transfer.at[l], in_sems.at[boxes + 3 + l])
        for l in range(levels)
    ]
    for l in range(local_levels):
        transfer_copies[l].start()
    for copy in signal_copies:
        copy.start()
    row_copy.start()

    barrier = pltpu.get_barrier_semaphore()
    for partner in partners:
        pl.semaphore_signal(barrier, inc=1, device_id=partner, device_id_type=MESH)
    for l in range(local_levels, levels):
        transfer_copies[l].start()
    block_copy.start()
    column_copy.start()

    source = lax.broadcasted_iota(jnp.int32, (LEAF, 4 * LEAF), 0)
    target = lax.broadcasted_iota(jnp.int32, (LEAF, 4 * LEAF), 1)
    group = target // LEAF
    child = group // 2
    lower = group % 2
    lane = target % LEAF
    inner = lane % wide
    imag = inner // rank
    moved = inner + lower * (rank - 2 * rank * imag)
    sign = (1 - 2 * imag * (1 - lower)).astype(F32)
    hit = source == child * wide + moved
    moves = [
        jnp.where(hit & (lane // wide == half), sign, 0.0).astype(BF16) for half in range(2)
    ]

    def build(l):
        transfer_copies[l].wait()
        forms = []
        for half in range(2):
            weights = transfer[l, half * pairs : (half + 1) * pairs].reshape(pairs * rank, LEAF)
            forms.append(dot(weights, moves[half]))
        if l == local_levels - 1:
            full = (forms[0] + forms[1]).astype(BF16).reshape(pairs, rank, 4 * LEAF)
            for g in range(4):
                spread[l, 0, :, g * rank : (g + 1) * rank, :] = full[
                    :, :, g * LEAF : (g + 1) * LEAF
                ]
            return
        for half in range(2):
            form = forms[half].astype(BF16).reshape(pairs, rank, 4 * LEAF)
            for c in range(2):
                for part in range(2):
                    top = half * wide + part * rank
                    g = 2 * c + part
                    spread[l, c, :, top : top + rank, :] = form[:, :, g * LEAF : (g + 1) * LEAF]

    left = lax.broadcasted_iota(jnp.int32, (rhs, LEAF), 1) < wide

    for l in range(local_levels):
        build(l)

    for copy in signal_copies:
        copy.wait()
    row_copy.wait()
    coeffs = []
    for k in range(pairs):
        real_side, imag_side = [], []
        for b in (k, k + pairs):
            basis = row_basis[:, b * LEAF : (b + 1) * LEAF]
            real_side += [basis[:rank], -basis[rank:]]
            imag_side += [basis[rank:], basis[:rank]]
        points = [win[2 * reach + b] for b in (k, k + pairs)]
        both = dot_t(
            jnp.concatenate([points[0][:rhs], points[1][:rhs]], axis=0),
            jnp.concatenate(real_side, axis=0),
        ) + dot_t(
            jnp.concatenate([points[0][rhs:], points[1][rhs:]], axis=0),
            jnp.concatenate(imag_side, axis=0),
        )
        coeffs.append(jnp.where(left, both[:rhs], both[rhs:]))

    pl.semaphore_wait(barrier, len(partners))
    halo = [
        pltpu.make_async_remote_copy(
            src_ref=win.at[pl.ds(boxes, 2 * reach)], dst_ref=win.at[pl.ds(0, 2 * reach)],
            send_sem=halo_send.at[0], recv_sem=halo_recv.at[0],
            device_id=next_id, device_id_type=MESH,
        ),
        pltpu.make_async_remote_copy(
            src_ref=win.at[pl.ds(2 * reach, 2 * reach)],
            dst_ref=win.at[pl.ds(2 * reach + boxes, 2 * reach)],
            send_sem=halo_send.at[1], recv_sem=halo_recv.at[1],
            device_id=prev_id, device_id_type=MESH,
        ),
    ]
    for copy in halo:
        copy.start()

    for l in range(local_levels - 1):
        bit = 1 << l
        coeffs = [
            product(coeffs[k & ~bit], spread[l, 0, k]) + product(coeffs[k | bit], spread[l, 1, k])
            for k in range(pairs)
        ]
    last = local_levels - 1
    coeffs = [product(coeffs[k], spread[last, 0, k]) for k in range(pairs)]

    chunk = pairs // CHUNKS

    def exchange(i, part):
        span = pl.ds(part * chunk, chunk)
        return pltpu.make_async_remote_copy(
            src_ref=sent.at[i, span], dst_ref=got.at[i, span],
            send_sem=send_sems.at[i, part], recv_sem=recv_sems.at[i, part],
            device_id=crossing[i][1], device_id_type=MESH,
        )

    def near_products():
        for copy in halo:
            copy.wait_recv()
        block_copy.wait()
        for s in range(slots):
            picked = win[jnp.maximum(list_ref[0, s], 0)]
            both = dot(picked, blocks[s])
            vals[s, :rhs] = both[:rhs, :LEAF] + both[rhs:, LEAF:]
            vals[s, rhs:] = both[rhs:, :LEAF] - both[:rhs, LEAF:]

    def near_sum(j):
        total = jnp.zeros((channels, LEAF), F32)
        for s in range(slots):
            total = total + jnp.where(list_ref[1, s] == j, vals[s], 0.0)
        near[j] = total

    def near_sums(first, stop):
        def body(j, carry):
            near_sum(j)
            return carry

        lax.fori_loop(first, stop, body, 0)

    rim = [
        pltpu.make_async_remote_copy(
            src_ref=near.at[pl.ds(0, reach)], dst_ref=edges.at[1],
            send_sem=halo_send.at[2], recv_sem=halo_recv.at[2],
            device_id=prev_id, device_id_type=MESH,
        ),
        pltpu.make_async_remote_copy(
            src_ref=near.at[pl.ds(boxes + reach, reach)], dst_ref=edges.at[0],
            send_sem=halo_send.at[3], recv_sem=halo_recv.at[3],
            device_id=next_id, device_id_type=MESH,
        ),
    ]

    def near_edges():
        near_products()
        near_sums(0, reach)
        rim[0].start()
        near_sums(boxes + reach, boxes + 2 * reach)
        rim[1].start()

    def near_middle():
        near_sums(reach, boxes + reach)

    def build_evals():
        column_copy.wait()
        for k in range(pairs):
            for half in range(2):
                b = k + half * pairs
                basis = column_basis[:, b * LEAF : (b + 1) * LEAF]
                top = half * wide
                evals[k, top : top + rank, :LEAF] = basis[:rank]
                evals[k, top : top + rank, LEAF:] = basis[rank:]
                evals[k, top + rank : top + wide, :LEAF] = -basis[rank:]
                evals[k, top + rank : top + wide, LEAF:] = basis[:rank]

    steps = len(crossing)
    extra = [[] for _ in range(steps)]
    extra[min(2, steps - 1)].append(near_edges)
    extra[min(3, steps - 1)].append(near_middle)
    extra[min(3, steps - 1)].append(build_evals)

    for part in range(CHUNKS):
        for k in range(part * chunk, (part + 1) * chunk):
            sent[0, k] = coeffs[k]
        exchange(0, part).start()
    for i in range(steps):
        l = local_levels + i
        bit = crossing[i][0]
        build(l)
        for k in range(pairs):
            own[k] = product(sent[i, k], spread[l, bit, k])
        for work in extra[i]:
            work()
        if i == steps - 1:
            for copy in rim:
                copy.wait_recv()
        for part in range(CHUNKS):
            exchange(i, part).wait_recv()
            for k in range(part * chunk, (part + 1) * chunk):
                value = own[k] + product(got[i, k], spread[l, 1 - bit, k])
                if i < steps - 1:
                    sent[i + 1, k] = value
                    continue
                high, low = halves(value)
                zero = jnp.zeros_like(high)
                far = dot(
                    jnp.concatenate(
                        [
                            jnp.where(left, high, zero), jnp.where(left, low, zero),
                            jnp.where(left, zero, high), jnp.where(left, zero, low),
                        ],
                        axis=0,
                    ),
                    evals[k],
                )
                for half in range(2):
                    b = k + half * pairs
                    both = far[2 * half * rhs : (2 * half + 1) * rhs] + far[
                        (2 * half + 1) * rhs : (2 * half + 2) * rhs
                    ]
                    result = near[reach + b]
                    if b < reach:
                        result = result + edges[0, b]
                    if b >= boxes - reach:
                        result = result + edges[1, b - boxes + reach]
                    here = slice(b * LEAF, (b + 1) * LEAF)
                    out_ref[:rhs, here] = both[:, :LEAF] + result[:rhs]
                    out_ref[rhs:, here] = both[:, LEAF:] + result[rhs:]
            if i < steps - 1:
                exchange(i + 1, part).start()
    for i in range(steps):
        for part in range(CHUNKS):
            exchange(i, part).wait_send()
    for copy in halo + rim:
        copy.wait_send()


def solution(mesh):
    leaf_count, sub_count = mesh.shape["leaf"], mesh.shape["sub"]
    steps = leaf_count.bit_length() + sub_count.bit_length() - 2

    def shards(signal, row_basis, transfer, column_basis, near_blocks, near_list):
        channels, points = signal.shape
        boxes = points // LEAF
        reach, pairs = boxes // 4, boxes // 2
        rhs = channels // 2
        levels, rank = transfer.shape[1], transfer.shape[2]
        slots = near_blocks.shape[0]
        anywhere = pl.BlockSpec(memory_space=pltpu.HBM)
        return pl.pallas_call(
            functools.partial(kernel, leaf_count, sub_count),
            out_shape=jax.ShapeDtypeStruct((channels, points), F32),
            in_specs=[pl.BlockSpec(memory_space=pltpu.SMEM)] + [anywhere] * 5,
            out_specs=pl.BlockSpec(memory_space=pltpu.VMEM),
            scratch_shapes=[
                pltpu.VMEM((boxes + 4 * reach, channels, LEAF), BF16),
                pltpu.VMEM(row_basis.shape, BF16),
                pltpu.VMEM((levels, boxes, rank, LEAF), BF16),
                pltpu.VMEM(column_basis.shape, BF16),
                pltpu.VMEM(near_blocks.shape, BF16),
                pltpu.VMEM((levels, 2, pairs, LEAF, LEAF), BF16),
                pltpu.VMEM((pairs, LEAF, 2 * LEAF), BF16),
                pltpu.VMEM((steps, pairs, rhs, LEAF), F32),
                pltpu.VMEM((steps, pairs, rhs, LEAF), F32),
                pltpu.VMEM((pairs, rhs, LEAF), F32),
                pltpu.VMEM((slots, channels, LEAF), F32),
                pltpu.VMEM((boxes + 2 * reach, channels, LEAF), F32),
                pltpu.VMEM((2, reach, channels, LEAF), F32),
                pltpu.SemaphoreType.DMA((boxes + 3 + levels,)),
                pltpu.SemaphoreType.DMA((steps, CHUNKS)),
                pltpu.SemaphoreType.DMA((steps, CHUNKS)),
                pltpu.SemaphoreType.DMA((4,)),
                pltpu.SemaphoreType.DMA((4,)),
            ],
            compiler_params=pltpu.CompilerParams(
                collective_id=0, has_side_effects=True, vmem_limit_bytes=63000000
            ),
        )(near_list.T, signal, row_basis, transfer, column_basis, near_blocks)

    return jax.shard_map(
        shards,
        mesh=mesh,
        in_specs=(
            P(None, ("leaf", "sub")),
            P(None, ("leaf", "sub")),
            P(("leaf", "sub"), None, None, None),
            P(None, ("leaf", "sub")),
            P(("leaf", "sub"), None, None),
            P(("leaf", "sub"), None),
        ),
        out_specs=P(None, ("leaf", "sub")),
        check_vma=False,
    )
```
